32 devices in a mesh: dp: 4 (over x, y), sp: 8 (over z, core).
Axes of the slice: x: 2, y: 2, z: 4, core: 2. Of those that a mesh axis runs over, the one named last changes fastest.
Arguments:
- x: bfloat16 [4096, 16384], P(('dp', 'sp')), parts along dimension 0
- gain: bfloat16 [16384], replicated
- wq: bfloat16 [16384, 16384], replicated
- wk: bfloat16 [16384, 16384], replicated
- wv: bfloat16 [16384, 16384], replicated
- wo: bfloat16 [16384, 16384], replicated
Outputs:
- output: bfloat16 [4096, 16384], P(('dp', 'sp')), parts along dimension 0
There are 4 independent parts. The reference program is written for one: setup_inputs(seed, part) draws one part's arguments, and reference() takes and returns one part's arrays. A program takes and returns all parts, laid end to end along the dimension named above; an argument that names none is the same for every part.
All inputs are finite; a program needn't handle non-finite values.
Results may differ from the reference program's by a relative error of at most 0.012.
Values are sent between devices in bfloat16 or wider.
A program may use at most 4.5 GiB of HBM per device.

```python
import jax
import jax.numpy as jnp
from jax import lax

ROWS = 1024
D = 16384
HEADS = 128
KV_HEADS = 128
HEAD = 128
THETA = 10000


def setup_inputs(seed: int = 0, part: int = 0) -> dict:
    kx, kn, kq, kk, kv, ko = jax.random.split(jax.random.key(seed), 6)

    def weights(key, rows, columns):
        return jax.random.normal(key, (rows, columns), jnp.float32) * rows**-0.5

    drawn = {
        "x": jax.random.normal(jax.random.fold_in(kx, part), (ROWS, D), jnp.float32),
        "gain": 1 + 0.1 * jax.random.normal(kn, (D,), jnp.float32),
        "wq": 2 * weights(kq, D, HEADS * HEAD),
        "wk": 2 * weights(kk, D, KV_HEADS * HEAD),
        "wv": 4 * weights(kv, D, KV_HEADS * HEAD),
        "wo": weights(ko, HEADS * HEAD, D),
    }
    return {k: v.astype(jnp.bfloat16) for k, v in drawn.items()}


def normed(x, gain):
    wide = x.astype(jnp.float32)
    scale = lax.rsqrt(jnp.mean(wide * wide, -1, keepdims=True) + 1e-6)
    return (wide * scale * gain.astype(jnp.float32)).astype(jnp.bfloat16)


def turned(t, place, theta):
    half = t.shape[-1] // 2
    angle = place.astype(jnp.float32)[:, None] * theta ** (-jnp.arange(half, dtype=jnp.float32) / half)
    cos, sin = jnp.cos(angle)[:, None], jnp.sin(angle)[:, None]
    a, b = t[..., :half].astype(jnp.float32), t[..., half:].astype(jnp.float32)
    return jnp.concatenate([a * cos - b * sin, b * cos + a * sin], -1).astype(jnp.bfloat16)


def matmul(a, w):
    return jnp.dot(a, w, preferred_element_type=jnp.float32).astype(jnp.bfloat16)


def einsum(form, a, b):
    return jnp.einsum(form, a.astype(jnp.float32), b.astype(jnp.float32))


def attention(q, k, v):
    scores = einsum("tgsd,ugd->gstu", q, k) * q.shape[-1] ** -0.5
    token = jnp.arange(q.shape[0])
    scores = jnp.where(token[:, None] >= token, scores, -jnp.inf)
    weights = jax.nn.softmax(scores, -1).astype(jnp.bfloat16)
    return einsum("gstu,ugd->tgsd", weights, v).astype(jnp.bfloat16)


def reference(x, gain, wq, wk, wv, wo):
    a, place = normed(x, gain), jnp.arange(ROWS)
    q = turned(matmul(a, wq).reshape(ROWS, HEADS, HEAD), place, THETA).reshape(ROWS, KV_HEADS, -1, HEAD)
    k = turned(matmul(a, wk).reshape(ROWS, KV_HEADS, HEAD), place, THETA)
    v = matmul(a, wv).reshape(ROWS, KV_HEADS, HEAD)
    seen = attention(q, k, v).reshape(ROWS, HEADS * HEAD)
    return (x.astype(jnp.float32) + jnp.dot(seen, wo, preferred_element_type=jnp.float32)).astype(jnp.bfloat16)
```

```python
import functools

import jax
import jax.numpy as jnp
from jax import lax
from jax.experimental import pallas as pl
from jax.experimental.pallas import tpu as pltpu
from jax.sharding import PartitionSpec as P

HEAD = 128
THETA = 10000
NEG = -1e30
HIDDEN = 2 * NEG
LOG2E = 1.4426950408889634
SCALE = HEAD**-0.5
MESH = pl.DeviceIdType.MESH
F32, BF16 = jnp.float32, jnp.bfloat16

ROWS = 128
CHIP = 2 * ROWS
GROUP = 2 * HEAD
SLOTS = 3
NQ = 8
NA = 2
NC = 6
LAGS = ((3, 1), (4, 2), (6, 0), (7, 1))
OUT = 2 * GROUP
NP = 4


def _dot(a, b, ca, cb):
    return lax.dot_general(a, b, (((ca,), (cb,)), ((), ())), preferred_element_type=F32)


def _parts(jobs):
    scores = []
    for q, kvs, _ in jobs:
        row = []
        for k, _, diagonal in kvs:
            s = _dot(k, q, 1, 1)
            if diagonal:
                s = jnp.where(lax.broadcasted_iota(jnp.int32, s.shape, 0) <= lax.broadcasted_iota(jnp.int32, s.shape, 1), s, HIDDEN)
            row.append(s)
        scores.append(row)
    weights = []
    for (_, _, carry), row in zip(jobs, scores):
        top = functools.reduce(jnp.maximum, [s.max(axis=0, keepdims=True) for s in row])
        keep = None
        if carry is not None:
            old = carry[1] * (1 / SCALE)
            top = jnp.maximum(top, old)
            keep = jnp.exp2((old - top) * (SCALE * LOG2E))
        row = [jnp.exp2((s - top) * (SCALE * LOG2E)) for s in row]
        total = sum(p.sum(axis=0, keepdims=True) for p in row)
        if carry is not None:
            total = total + keep
        weights.append(([p.astype(BF16) for p in row], keep, total, top))
    got = []
    for (_, kvs, carry), (row, keep, total, top) in zip(jobs, weights):
        out = sum(_dot(vt, p, 1, 0) for (_, vt, _), p in zip(kvs, row))
        if carry is not None:
            out = out + carry[0].astype(F32) * keep
        got.append((out * (1 / total), top * SCALE + jnp.log(total)))
    return got


def _kernel(x_hbm, gain_ref, cos_ref, sin_ref, wq, wk, wv, wo, y_hbm, a_ref, wbuf, seen, qring, kring, vring, rkv, cin_o, cin_l, cout_o, cout_l,
            acc, pacc, prec, ybuf, wsem, xsem, axs, axr, qs, qr, cso, csl, cro, crl, as_, ar, ps, pr, ysem, x2sem):
    dim = x_hbm.shape[1]
    half = dim // 2
    ng, nw = half // GROUP, dim // OUT
    me, dp = lax.axis_index("sp"), lax.axis_index("dp")
    z, core = lax.div(me, 2), lax.rem(me, 2)
    up, down, partner = me + 2, me - 2, me + 1 - 2 * core
    own_rows = pl.multiple_of(core * ROWS, ROWS)
    other_rows = pl.multiple_of((1 - core) * ROWS, ROWS)
    halves = [pl.ds(h * HEAD, HEAD) for h in range(2)]

    def remote(src, dst, send, recv, target):
        return pltpu.make_async_remote_copy(src, dst, send, recv, device_id=(dp, target), device_id_type=MESH)

    n1 = nw // 2
    k1 = max(ng - 8, 1) * GROUP
    k2 = half - k1
    done = 3 * ng

    def fetch(w, g, i):
        slot = lax.rem(i, SLOTS)
        col = pl.multiple_of(core * half + g * GROUP, GROUP)
        pltpu.make_async_copy(w.at[:, pl.ds(col, GROUP)], wbuf.at[slot], wsem.at[slot]).start()

    def fetch_out(i, n, first, depth):
        slot = lax.rem(i, SLOTS)
        rows = pl.ds(pl.multiple_of(core * half + first, GROUP), depth)
        for j in range(2):
            col = pl.multiple_of(n * OUT + j * GROUP, GROUP)
            pltpu.make_async_copy(wo.at[rows, pl.ds(col, GROUP)], wbuf.at[slot, pl.ds(j * depth, depth), :], wsem.at[slot]).start()

    def fetch_first(n):
        fetch_out(done + n, n, 0, k1)

    def fetch_full(r):
        fetch_out(done + n1 + 2 * r, n1 + r, 0, half)

    def fetch_rest(r):
        fetch_out(done + n1 + 2 * r + 1, r, k1, k2)

    def fetch_after(i):
        pl.when(i < n1)(lambda: fetch_first(i))
        pl.when(i == n1)(lambda: fetch_full(0))
        pl.when(i == n1 + 1)(lambda: fetch_rest(0))

    def arrived(i, rows):
        slot = lax.rem(i, SLOTS)
        pltpu.make_async_copy(wq.at[pl.ds(0, rows), pl.ds(0, GROUP)], wbuf.at[slot, pl.ds(0, rows), :], wsem.at[slot]).wait()
        return slot

    step_rows = ROWS // 4

    def x_copy(c):
        return pltpu.make_async_copy(x_hbm.at[pl.ds(c * step_rows, step_rows), :],
                                     a_ref.at[pl.ds(own_rows + c * step_rows, step_rows), :], xsem.at[c])

    def a_copy(c):
        rows = pl.ds(pl.multiple_of(own_rows + c * step_rows, step_rows), step_rows)
        return remote(a_ref.at[rows, :], a_ref.at[rows, :], axs.at[c], axr.at[c], partner)

    for c in range(4):
        x_copy(c).start()
    for j, w in enumerate((wq, wk, wv)):
        fetch(w, 0, j)

    barrier = pltpu.get_barrier_semaphore()
    pl.semaphore_signal(barrier, inc=1, device_id=(dp, partner), device_id_type=MESH)

    @pl.when(z > 0)
    def _():
        pl.semaphore_signal(barrier, inc=1, device_id=(dp, down), device_id_type=MESH)

    @pl.when(z < 3)
    def _():
        pl.semaphore_signal(barrier, inc=1, device_id=(dp, up), device_id_type=MESH)

    ends = (z == 0) | (z == 3)

    @pl.when(ends)
    def _():
        pl.semaphore_wait(barrier, 2)

    @pl.when(~ends)
    def _():
        pl.semaphore_wait(barrier, 3)

    cout_l[...] = jnp.zeros(cout_l.shape, F32)

    def norm(c, _):
        x_copy(c).wait()

        def rows16(r, _):
            rows = pl.ds(pl.multiple_of(own_rows + c * step_rows + r * 16, 16), 16)
            wide = a_ref[rows, :].astype(F32)
            scale = lax.rsqrt(jnp.mean(wide * wide, -1, keepdims=True) + 1e-6)
            a_ref[rows, :] = (wide * scale * gain_ref[...].astype(F32)).astype(BF16)

        lax.fori_loop(0, step_rows // 16, rows16, None)
        a_copy(c).start()

    lax.fori_loop(0, 4, norm, None)
    for c in range(4):
        a_copy(c).wait_send()
        a_copy(c).wait_recv()

    def is_a(g):
        return (g >= 0) & (g < ng) & (lax.rem(g + 3, 3) == 1)

    def is_b(g):
        return (g >= 0) & (g < ng) & (lax.rem(g + 3, 3) != 1)

    def q_copy(slot, t):
        return remote(qring.at[slot, t], qring.at[slot, t + 1], qs.at[slot, t], qr.at[slot, t], down)

    def k_copy(slot, n):
        return remote(kring.at[slot], rkv.at[n, 0, 0], as_.at[n, 0, 0], ar.at[n, 0, 0], up)

    def v_copy(slot, n):
        return remote(vring.at[slot], rkv.at[n, 0, 1], as_.at[n, 0, 1], ar.at[n, 0, 1], up)

    def kv_copy(n, d, j):
        return remote(rkv.at[n, max(d, 1) - 1, j], rkv.at[n, d, j], as_.at[n, d, j], ar.at[n, d, j], up)

    def part_copies(m, c, t):
        return (remote(cout_o.at[m, t - 1], cin_o.at[c, t - 1], cso.at[m, t - 1], cro.at[c, t - 1], up),
                remote(cout_l.at[m, t - 1], cin_l.at[c, t - 1], csl.at[m, t - 1], crl.at[c, t - 1], up))

    def a_place(g):
        return lax.rem(lax.div(g + 2, 3) - 1, NA)

    def b_place(g):
        return g - lax.div(g + 1, 3)

    def tile(s, m):
        i = 3 * s + m
        slot = arrived(i, dim)
        got = jnp.dot(a_ref[...], wbuf[slot], preferred_element_type=F32).astype(BF16)
        place = lax.rem(s, NQ)
        if m == 2:
            vring[place] = got.T
        else:
            for h in halves:
                t = got[:, h.start : h.start + HEAD].astype(F32)
                t = t * cos_ref[...] + pltpu.roll(t, HEAD // 2, 1) * sin_ref[...]
                if m == 0:
                    qring[place, 0, :, h] = t.astype(BF16)
                else:
                    kring[place, :, h] = t.astype(BF16)
        if m == 0:
            @pl.when(is_b(s) & (z > 0))
            def _():
                q_copy(place, 0).start()
        else:
            @pl.when(is_a(s) & (z < 3))
            def _():
                (k_copy if m == 1 else v_copy)(place, a_place(s)).start()

    def relay_b(g, t):
        @pl.when(is_b(g) & (z < 4 - t))
        def _():
            place = lax.rem(g, NQ)
            q_copy(place, t - 1).wait_recv()

            @pl.when(z > 0)
            def _():
                q_copy(place, t).start()

    def relay_a(g, d):
        @pl.when(is_a(g) & (z >= d))
        def _():
            n = a_place(g)
            for j in range(2):
                kv_copy(n, d - 1, j).wait_recv()

            @pl.when(z < 3)
            def _():
                for j in range(2):
                    kv_copy(n, d, j).start()

    def finish(g, h, out):
        cols = pl.ds(pl.multiple_of(g * GROUP + h.start, HEAD), HEAD)
        seen[:, cols] = out.T.astype(BF16)

    def attend_b(g, at):
        place, b = lax.rem(g, NQ), b_place(g)
        m, c = lax.rem(b, 2), lax.rem(b, NC)
        tiles = range(3 - at, -1, -1)
        if at > 0:
            for t in tiles:
                q_copy(place, t).wait_send()
        else:
            q_copy(place, 2).wait_recv()
        for t in tiles:
            if at > 0:
                for copy in part_copies(m, c, t + 1):
                    copy.wait_recv()
            if t > 0:
                @pl.when(b >= 2)
                def _():
                    for copy in part_copies(m, c, t):
                        copy.wait_send()

        jobs = []
        for t in tiles:
            for j, h in enumerate(halves):
                carry = (cin_o[c, t, h, :], cin_l[c, t, j : j + 1, :]) if at > 0 else None
                jobs.append((qring[place, t, :, h], [(kring[place, :, h], vring[place, h, :], t == 0)], carry))
        got = iter(_parts(jobs))
        for t in tiles:
            for j, h in enumerate(halves):
                out, lse = next(got)
                if t == 0:
                    finish(g, h, out)
                else:
                    cout_o[m, t - 1, h, :] = out.astype(BF16)
                    cout_l[m, t - 1, j : j + 1, :] = lse
        for t in tiles:
            if t > 0:
                for copy in part_copies(m, c, t):
                    copy.start()

    def attend_a(g, at):
        place, n = lax.rem(g, NQ), a_place(g)
        if at < 3:
            k_copy(place, n).wait_send()
            v_copy(place, n).wait_send()
            for d in range(1, at + 1):
                for j in range(2):
                    kv_copy(n, d, j).wait_send()
        else:
            for j in range(2):
                kv_copy(n, 2, j).wait_recv()
        jobs = []
        for h in halves:
            kvs = [(kring[place, :, h], vring[place, h, :], True)]
            kvs += [(rkv[n, d, 0, :, h], rkv[n, d, 1, h, :], False) for d in range(at)]
            jobs.append((qring[place, 0, :, h], kvs, None))
        for h, (out, _) in zip(halves, _parts(jobs)):
            finish(g, h, out)

    def first_step(n):
        slot = arrived(done + n, 2 * k1)
        for j in range(2):
            acc[n, :, j * GROUP : (j + 1) * GROUP] = jnp.dot(seen[:, 0:k1], wbuf[slot, j * k1 : (j + 1) * k1, :], preferred_element_type=F32)

    def iteration(s, _):
        for m in range(3):
            ahead, kind = s + (m + 2) // 3, (m + 2) % 3

            @pl.when((ahead < ng) & (s > 0) if m == 0 else ahead < ng)
            def _():
                fetch((wq, wk, wv)[kind], ahead, 3 * s + m + 2)

            @pl.when(ahead >= ng)
            def _():
                fetch_after(3 * (ahead - ng) + kind)

            @pl.when(s < ng)
            def _():
                tile(s, m)

            @pl.when((s >= ng) & (3 * (s - ng) + m < n1))
            def _():
                first_step(3 * (s - ng) + m)

            if m == 0:
                relay_b(s - 1, 1)
                relay_b(s - 2, 2)
            if m == 2:
                relay_a(s - 1, 1)
                relay_a(s - 2, 2)
            for at, (lag, when) in enumerate(LAGS):
                if m == when:
                    pl.when((z == at) & is_b(s - lag))(functools.partial(attend_b, s - lag, at))
                if m == 2:
                    pl.when((z == at) & is_a(s - 3))(functools.partial(attend_a, s - 3, at))

    lax.fori_loop(0, ng + LAGS[3][0], iteration, None)

    nb = ng - (ng + 1) // 3
    for b in (nb - 2, nb - 1):
        for t in (1, 2, 3):
            @pl.when(z <= 3 - t)
            def _():
                for copy in part_copies(b % 2, b % NC, t):
                    copy.wait_send()

    x_again = pltpu.make_async_copy(x_hbm, a_ref.at[pl.ds(0, ROWS), :], x2sem)
    x_again.start()

    def columns(j):
        n = lax.div(j, 2) + jnp.where(lax.rem(j, 2) == 0, n1, 0)
        return pl.ds(pl.multiple_of(n * OUT, OUT), OUT)

    def sums(j):
        p = lax.rem(j, NP)
        return remote(pacc.at[p, pl.ds(other_rows, ROWS), :], prec.at[p], ps.at[p], pr.at[p], partner)

    def y_copy(j):
        p = lax.rem(j + 2, 2)
        return pltpu.make_async_copy(ybuf.at[p], y_hbm.at[:, columns(j)], ysem.at[p])

    def finalize(j):
        p = lax.rem(j, NP)
        sums(j).wait_send()
        sums(j).wait_recv()

        @pl.when(j >= 2)
        def _():
            y_copy(j - 2).wait()

        x = a_ref[0:ROWS, columns(j)].astype(F32)
        ybuf[lax.rem(j, 2)] = (x + (pacc[p, pl.ds(own_rows, ROWS), :] + prec[p])).astype(BF16)
        y_copy(j).start()

    def out_pair(r, _):
        @pl.when(r + 1 < n1)
        def _():
            fetch_full(r + 1)

        slot = arrived(done + n1 + 2 * r, dim)
        p = lax.rem(2 * r, NP)
        for j in range(2):
            pacc[p, :, j * GROUP : (j + 1) * GROUP] = jnp.dot(seen[...], wbuf[slot, j * half : (j + 1) * half, :], preferred_element_type=F32)
        sums(2 * r).start()

        @pl.when(r == 0)
        def _():
            x_again.wait()

        @pl.when(r > 0)
        def _():
            finalize(2 * r - 1)

        @pl.when(r + 1 < n1)
        def _():
            fetch_rest(r + 1)

        slot = arrived(done + n1 + 2 * r + 1, 2 * k2)
        p = lax.rem(2 * r + 1, NP)
        for j in range(2):
            cols = slice(j * GROUP, (j + 1) * GROUP)
            pacc[p, :, cols] = acc[r, :, cols] + jnp.dot(seen[:, k1:half], wbuf[slot, j * k2 : (j + 1) * k2, :], preferred_element_type=F32)
        sums(2 * r + 1).start()
        finalize(2 * r)

    lax.fori_loop(0, n1, out_pair, None)
    finalize(nw - 1)
    for j in (nw - 2, nw - 1):
        y_copy(j).wait()


def _layer(x, gain, cos, sin, wq, wk, wv, wo):
    rows, dim = x.shape
    vmem, hbm = pl.BlockSpec(memory_space=pltpu.VMEM), pl.BlockSpec(memory_space=pl.ANY)
    sem = pltpu.SemaphoreType.DMA
    return pl.pallas_call(
        _kernel,
        out_shape=jax.ShapeDtypeStruct((rows, dim), BF16),
        in_specs=[hbm, vmem, vmem, vmem, hbm, hbm, hbm, hbm],
        out_specs=hbm,
        scratch_shapes=[
            pltpu.VMEM((CHIP, dim), BF16),
            pltpu.VMEM((SLOTS, dim, GROUP), BF16),
            pltpu.VMEM((CHIP, dim // 2), BF16),
            pltpu.VMEM((NQ, 4, CHIP, GROUP), BF16),
            pltpu.VMEM((NQ, CHIP, GROUP), BF16),
            pltpu.VMEM((NQ, GROUP, CHIP), BF16),
            pltpu.VMEM((NA, 3, 2, CHIP, GROUP), BF16),
            pltpu.VMEM((NC, 3, GROUP, CHIP), BF16),
            pltpu.VMEM((NC, 3, 8, CHIP), F32),
            pltpu.VMEM((2, 3, GROUP, CHIP), BF16),
            pltpu.VMEM((2, 3, 8, CHIP), F32),
            pltpu.VMEM((dim // OUT // 2, CHIP, OUT), F32),
            pltpu.VMEM((NP, CHIP, OUT), F32),
            pltpu.VMEM((NP, ROWS, OUT), F32),
            pltpu.VMEM((2, ROWS, OUT), BF16),
            sem((SLOTS,)), sem((4,)), sem((4,)), sem((4,)),
            sem((NQ, 3)), sem((NQ, 3)),
            sem((2, 3)), sem((2, 3)), sem((NC, 3)), sem((NC, 3)),
            sem((NA, 3, 2)), sem((NA, 3, 2)),
            sem((NP,)), sem((NP,)), sem((2,)), sem,
        ],
        compiler_params=pltpu.CompilerParams(collective_id=0, has_side_effects=True, vmem_limit_bytes=67043328),
        name="layer",
    )(x, gain, cos, sin, wq, wk, wv, wo)


def solution(mesh):
    def step(x, gain, wq, wk, wv, wo):
        place = lax.div(lax.axis_index("sp"), 2) * CHIP + jnp.arange(CHIP)
        angle = place.astype(F32)[:, None] * THETA ** (-jnp.arange(HEAD // 2, dtype=F32) / (HEAD // 2))
        cos, sin = jnp.cos(angle), jnp.sin(angle)
        return _layer(x, gain[None], jnp.concatenate([cos, cos], 1), jnp.concatenate([-sin, sin], 1), wq, wk, wv, wo)

    tokens, whole = P(("dp", "sp"), None), P(None, None)
    return jax.shard_map(step, mesh=mesh, in_specs=(tokens, P(None), whole, whole, whole, whole), out_specs=tokens, check_vma=False)
```

```python
import functools

import jax
import jax.numpy as jnp
from jax import lax
from jax.experimental import pallas as pl
from jax.experimental.pallas import tpu as pltpu
from jax.sharding import PartitionSpec as P

HEAD = 128
THETA = 10000
NEG = -1e30
HIDDEN = 2 * NEG
LOG2E = 1.4426950408889634
SCALE = HEAD**-0.5
MESH = pl.DeviceIdType.MESH
F32, BF16 = jnp.float32, jnp.bfloat16

ROWS = 128
CHIP = 2 * ROWS
GROUP = 2 * HEAD
SLOTS = 3
NQ = 8
NA = 2
NC = 6
LAGS, LAG_A = ((3, 2), (5, 0), (6, 1), (7, 2)), (4, 0)
OUT = 2 * GROUP
NP = 4


def _dot(a, b, ca, cb):
    return lax.dot_general(a, b, (((ca,), (cb,)), ((), ())), preferred_element_type=F32)


def _parts(jobs):
    scores = []
    for q, kvs, _ in jobs:
        row = []
        for k, _, diagonal in kvs:
            s = _dot(k, q, 1, 1)
            if diagonal:
                s = jnp.where(lax.broadcasted_iota(jnp.int32, s.shape, 0) <= lax.broadcasted_iota(jnp.int32, s.shape, 1), s, HIDDEN)
            row.append(s)
        scores.append(row)
    weights = []
    for (_, _, carry), row in zip(jobs, scores):
        top = functools.reduce(jnp.maximum, [s.max(axis=0, keepdims=True) for s in row])
        keep = None
        if carry is not None:
            old = carry[1] * (1 / SCALE)
            top = jnp.maximum(top, old)
            keep = jnp.exp2((old - top) * (SCALE * LOG2E))
        row = [jnp.exp2((s - top) * (SCALE * LOG2E)) for s in row]
        total = sum(p.sum(axis=0, keepdims=True) for p in row)
        if carry is not None:
            total = total + keep
        weights.append(([p.astype(BF16) for p in row], keep, total, top))
    got = []
    for (_, kvs, carry), (row, keep, total, top) in zip(jobs, weights):
        out = sum(_dot(vt, p, 1, 0) for (_, vt, _), p in zip(kvs, row))
        if carry is not None:
            out = out + carry[0].astype(F32) * keep
        got.append((out * (1 / total), top * SCALE + jnp.log(total)))
    return got


def _kernel(x_hbm, gain_ref, cos_ref, sin_ref, wq, wk, wv, wo, y_hbm, a_ref, wbuf, seen, qring, kring, vring, rkv, cin_o, cin_l, cout_o, cout_l,
            prod, acc, pacc, prec, ybuf, wsem, xsem, axs, axr, qs, qr, cso, csl, cro, crl, as_, ar, ps, pr, ysem, x2sem):
    dim = x_hbm.shape[1]
    half = dim // 2
    ng, nw = half // GROUP, dim // OUT
    me, dp = lax.axis_index("sp"), lax.axis_index("dp")
    z, core = lax.div(me, 2), lax.rem(me, 2)
    up, down, partner = me + 2, me - 2, me + 1 - 2 * core
    own_rows = pl.multiple_of(core * ROWS, ROWS)
    other_rows = pl.multiple_of((1 - core) * ROWS, ROWS)
    halves = [pl.ds(h * HEAD, HEAD) for h in range(2)]

    def remote(src, dst, send, recv, target):
        return pltpu.make_async_remote_copy(src, dst, send, recv, device_id=(dp, target), device_id_type=MESH)

    n1 = nw // 2
    k1 = max(ng - 8, 1) * GROUP
    k2 = half - k1
    done = 3 * ng

    def fetch(w, g, i):
        slot = lax.rem(i, SLOTS)
        col = pl.multiple_of(core * half + g * GROUP, GROUP)
        pltpu.make_async_copy(w.at[:, pl.ds(col, GROUP)], wbuf.at[slot], wsem.at[slot]).start(priority=1)

    def fetch_out(i, n, first, depth):
        slot = lax.rem(i, SLOTS)
        rows = pl.ds(pl.multiple_of(core * half + first, GROUP), depth)
        for j in range(2):
            col = pl.multiple_of(n * OUT + j * GROUP, GROUP)
            pltpu.make_async_copy(wo.at[rows, pl.ds(col, GROUP)], wbuf.at[slot, pl.ds(j * depth, depth), :], wsem.at[slot]).start(priority=1)

    def fetch_first(n):
        fetch_out(done + n, n, 0, k1)

    def fetch_full(r):
        fetch_out(done + n1 + 2 * r, n1 + r, 0, half)

    def fetch_rest(r):
        fetch_out(done + n1 + 2 * r + 1, r, k1, k2)

    def fetch_after(i):
        pl.when(i < n1)(lambda: fetch_first(i))
        pl.when(i == n1)(lambda: fetch_full(0))
        pl.when(i == n1 + 1)(lambda: fetch_rest(0))

    def arrived(i, rows):
        slot = lax.rem(i, SLOTS)
        pltpu.make_async_copy(wq.at[pl.ds(0, rows), pl.ds(0, GROUP)], wbuf.at[slot, pl.ds(0, rows), :], wsem.at[slot]).wait()
        return slot

    step_rows = ROWS // 4

    def x_copy(c):
        return pltpu.make_async_copy(x_hbm.at[pl.ds(c * step_rows, step_rows), :],
                                     a_ref.at[pl.ds(own_rows + c * step_rows, step_rows), :], xsem.at[c])

    def a_copy(c):
        rows = pl.ds(pl.multiple_of(own_rows + c * step_rows, step_rows), step_rows)
        return remote(a_ref.at[rows, :], a_ref.at[rows, :], axs.at[c], axr.at[c], partner)

    for c in range(4):
        x_copy(c).start()
    for j, w in enumerate((wq, wk, wv)):
        fetch(w, 0, j)

    barrier = pltpu.get_barrier_semaphore()
    pl.semaphore_signal(barrier, inc=1, device_id=(dp, partner), device_id_type=MESH)

    @pl.when(z > 0)
    def _():
        pl.semaphore_signal(barrier, inc=1, device_id=(dp, down), device_id_type=MESH)

    @pl.when(z < 3)
    def _():
        pl.semaphore_signal(barrier, inc=1, device_id=(dp, up), device_id_type=MESH)

    ends = (z == 0) | (z == 3)

    @pl.when(ends)
    def _():
        pl.semaphore_wait(barrier, 2)

    @pl.when(~ends)
    def _():
        pl.semaphore_wait(barrier, 3)

    cout_l[...] = jnp.zeros(cout_l.shape, F32)
    prod[...] = jnp.zeros(prod.shape, BF16)

    def norm(c, _):
        x_copy(c).wait()

        def rows16(r, _):
            rows = pl.ds(pl.multiple_of(own_rows + c * step_rows + r * 16, 16), 16)
            wide = a_ref[rows, :].astype(F32)
            scale = lax.rsqrt(jnp.mean(wide * wide, -1, keepdims=True) + 1e-6)
            a_ref[rows, :] = (wide * scale * gain_ref[...].astype(F32)).astype(BF16)

        lax.fori_loop(0, step_rows // 16, rows16, None)
        a_copy(c).start()

    lax.fori_loop(0, 4, norm, None)
    for c in range(4):
        a_copy(c).wait_send()
        a_copy(c).wait_recv()

    def is_a(g):
        return (g >= 0) & (g < ng) & (lax.rem(g + 3, 3) == 1)

    def is_b(g):
        return (g >= 0) & (g < ng) & (lax.rem(g + 3, 3) != 1)

    def q_copy(slot, t):
        return remote(qring.at[slot, t], qring.at[slot, t + 1], qs.at[slot, t], qr.at[slot, t], down)

    def k_copy(slot, n):
        return remote(kring.at[slot], rkv.at[n, 0, 0], as_.at[n, 0, 0], ar.at[n, 0, 0], up)

    def v_copy(slot, n):
        return remote(vring.at[slot], rkv.at[n, 0, 1], as_.at[n, 0, 1], ar.at[n, 0, 1], up)

    def kv_copy(n, d, j):
        return remote(rkv.at[n, max(d, 1) - 1, j], rkv.at[n, d, j], as_.at[n, d, j], ar.at[n, d, j], up)

    def part_copies(m, c, t):
        return (remote(cout_o.at[m, t - 1], cin_o.at[c, t - 1], cso.at[m, t - 1], cro.at[c, t - 1], up),
                remote(cout_l.at[m, t - 1], cin_l.at[c, t - 1], csl.at[m, t - 1], crl.at[c, t - 1], up))

    def a_place(g):
        return lax.rem(lax.div(g + 2, 3) - 1, NA)

    def b_place(g):
        return g - lax.div(g + 1, 3)

    def keep(g, m):
        place = lax.rem(g + NQ, NQ)
        if m == 2:
            vring[place] = prod[...].T
        else:
            for h in halves:
                t = prod[:, h].astype(F32)
                t = t * cos_ref[...] + pltpu.roll(t, HEAD // 2, 1) * sin_ref[...]
                if m == 0:
                    qring[place, 0, :, h] = t.astype(BF16)
                else:
                    kring[place, :, h] = t.astype(BF16)

    def send_kept(g, m):
        place = lax.rem(g + NQ, NQ)
        if m == 0:
            @pl.when(is_b(g) & (z > 0))
            def _():
                q_copy(place, 0).start()
        else:
            @pl.when(is_a(g) & (z < 3))
            def _():
                (k_copy if m == 1 else v_copy)(place, a_place(g)).start()

    def tile(s, m):
        i = 3 * s + m
        slot = arrived(i, dim)
        g, before = s - (m == 0), (m + 2) % 3
        keep(g, before)
        prod[...] = jnp.dot(a_ref[...], wbuf[slot], preferred_element_type=F32).astype(BF16)
        send_kept(g, before)

    def relay_b(g, t):
        @pl.when(is_b(g) & (z < 4 - t))
        def _():
            place = lax.rem(g, NQ)
            q_copy(place, t - 1).wait_recv()

            @pl.when(z > 0)
            def _():
                q_copy(place, t).start()

    def relay_a(g, d):
        @pl.when(is_a(g) & (z >= d))
        def _():
            n = a_place(g)
            for j in range(2):
                kv_copy(n, d - 1, j).wait_recv()

            @pl.when(z < 3)
            def _():
                for j in range(2):
                    kv_copy(n, d, j).start()

    def finish(g, h, out):
        cols = pl.ds(pl.multiple_of(g * GROUP + h.start, HEAD), HEAD)
        seen[:, cols] = out.T.astype(BF16)

    def attend_b(g, at):
        place, b = lax.rem(g, NQ), b_place(g)
        m, c = lax.rem(b, 2), lax.rem(b, NC)
        tiles = range(3 - at, -1, -1)
        if at > 0:
            for t in tiles:
                q_copy(place, t).wait_send()
        else:
            q_copy(place, 2).wait_recv()
        for t in tiles:
            if at > 0:
                for copy in part_copies(m, c, t + 1):
                    copy.wait_recv()
            if t > 0:
                @pl.when(b >= 2)
                def _():
                    for copy in part_copies(m, c, t):
                        copy.wait_send()

        jobs = []
        for t in tiles:
            for j, h in enumerate(halves):
                carry = (cin_o[c, t, h, :], cin_l[c, t, j : j + 1, :]) if at > 0 else None
                jobs.append((qring[place, t, :, h], [(kring[place, :, h], vring[place, h, :], t == 0)], carry))
        got = iter(_parts(jobs))
        for t in tiles:
            for j, h in enumerate(halves):
                out, lse = next(got)
                if t == 0:
                    finish(g, h, out)
                else:
                    cout_o[m, t - 1, h, :] = out.astype(BF16)
                    cout_l[m, t - 1, j : j + 1, :] = lse
        for t in tiles:
            if t > 0:
                for copy in part_copies(m, c, t):
                    copy.start()

    def attend_a(g, at):
        place, n = lax.rem(g, NQ), a_place(g)
        if at < 3:
            k_copy(place, n).wait_send()
            v_copy(place, n).wait_send()
            for d in range(1, at + 1):
                for j in range(2):
                    kv_copy(n, d, j).wait_send()
        else:
            for j in range(2):
                kv_copy(n, 2, j).wait_recv()
        jobs = []
        for h in halves:
            kvs = [(kring[place, :, h], vring[place, h, :], True)]
            kvs += [(rkv[n, d, 0, :, h], rkv[n, d, 1, h, :], False) for d in range(at)]
            jobs.append((qring[place, 0, :, h], kvs, None))
        for h, (out, _) in zip(halves, _parts(jobs)):
            finish(g, h, out)

    def first_step(n):
        slot = arrived(done + n, 2 * k1)
        for j in range(2):
            acc[n, :, j * GROUP : (j + 1) * GROUP] = jnp.dot(seen[:, 0:k1], wbuf[slot, j * k1 : (j + 1) * k1, :], preferred_element_type=F32)

    def iteration(s, _):
        for m in range(3):
            ahead, kind = s + (m + 2) // 3, (m + 2) % 3

            @pl.when((ahead < ng) & (s > 0) if m == 0 else ahead < ng)
            def _():
                fetch((wq, wk, wv)[kind], ahead, 3 * s + m + 2)

            @pl.when(ahead >= ng)
            def _():
                fetch_after(3 * (ahead - ng) + kind)

            @pl.when(s < ng)
            def _():
                tile(s, m)

            @pl.when((s >= ng) & (3 * (s - ng) + m < n1))
            def _():
                first_step(3 * (s - ng) + m)

            if m == 0:
                @pl.when(s == ng)
                def _():
                    keep(ng - 1, 2)
                    send_kept(ng - 1, 2)

                relay_a(s - 2, 1)
                relay_a(s - 3, 2)
            if m == 1:
                relay_b(s - 1, 1)
                relay_b(s - 2, 2)
            for at, (lag, when) in enumerate(LAGS):
                if m == when:
                    pl.when((z == at) & is_b(s - lag))(functools.partial(attend_b, s - lag, at))
                if m == LAG_A[1]:
                    pl.when((z == at) & is_a(s - LAG_A[0]))(functools.partial(attend_a, s - LAG_A[0], at))

    lax.fori_loop(0, ng + LAGS[3][0], iteration, None)

    nb = ng - (ng + 1) // 3
    for b in (nb - 2, nb - 1):
        for t in (1, 2, 3):
            @pl.when(z <= 3 - t)
            def _():
                for copy in part_copies(b % 2, b % NC, t):
                    copy.wait_send()

    x_again = pltpu.make_async_copy(x_hbm, a_ref.at[pl.ds(0, ROWS), :], x2sem)
    x_again.start()

    def columns(j):
        n = lax.div(j, 2) + jnp.where(lax.rem(j, 2) == 0, n1, 0)
        return pl.ds(pl.multiple_of(n * OUT, OUT), OUT)

    def sums(j):
        p = lax.rem(j, NP)
        return remote(pacc.at[p, pl.ds(other_rows, ROWS), :], prec.at[p], ps.at[p], pr.at[p], partner)

    def y_copy(j):
        p = lax.rem(j + 2, 2)
        return pltpu.make_async_copy(ybuf.at[p], y_hbm.at[:, columns(j)], ysem.at[p])

    def finalize(j):
        p = lax.rem(j, NP)
        sums(j).wait_send()
        sums(j).wait_recv()

        @pl.when(j >= 2)
        def _():
            y_copy(j - 2).wait()

        x = a_ref[0:ROWS, columns(j)].astype(F32)
        ybuf[lax.rem(j, 2)] = (x + (pacc[p, pl.ds(own_rows, ROWS), :] + prec[p])).astype(BF16)
        y_copy(j).start()

    def out_pair(r, _):
        @pl.when(r + 1 < n1)
        def _():
            fetch_full(r + 1)

        slot = arrived(done + n1 + 2 * r, dim)
        p = lax.rem(2 * r, NP)
        for j in range(2):
            pacc[p, :, j * GROUP : (j + 1) * GROUP] = jnp.dot(seen[...], wbuf[slot, j * half : (j + 1) * half, :], preferred_element_type=F32)
        sums(2 * r).start()

        @pl.when(r == 0)
        def _():
            x_again.wait()

        @pl.when(r > 0)
        def _():
            finalize(2 * r - 1)

        @pl.when(r + 1 < n1)
        def _():
            fetch_rest(r + 1)

        slot = arrived(done + n1 + 2 * r + 1, 2 * k2)
        p = lax.rem(2 * r + 1, NP)
        for j in range(2):
            cols = slice(j * GROUP, (j + 1) * GROUP)
            pacc[p, :, cols] = acc[r, :, cols] + jnp.dot(seen[:, k1:half], wbuf[slot, j * k2 : (j + 1) * k2, :], preferred_element_type=F32)
        sums(2 * r + 1).start()
        finalize(2 * r)

    lax.fori_loop(0, n1, out_pair, None)
    finalize(nw - 1)
    for j in (nw - 2, nw - 1):
        y_copy(j).wait()


def _layer(x, gain, cos, sin, wq, wk, wv, wo):
    rows, dim = x.shape
    vmem, hbm = pl.BlockSpec(memory_space=pltpu.VMEM), pl.BlockSpec(memory_space=pl.ANY)
    sem = pltpu.SemaphoreType.DMA
    return pl.pallas_call(
        _kernel,
        out_shape=jax.ShapeDtypeStruct((rows, dim), BF16),
        in_specs=[hbm, vmem, vmem, vmem, hbm, hbm, hbm, hbm],
        out_specs=hbm,
        scratch_shapes=[
            pltpu.VMEM((CHIP, dim), BF16),
            pltpu.VMEM((SLOTS, dim, GROUP), BF16),
            pltpu.VMEM((CHIP, dim // 2), BF16),
            pltpu.VMEM((NQ, 4, CHIP, GROUP), BF16),
            pltpu.VMEM((NQ, CHIP, GROUP), BF16),
            pltpu.VMEM((NQ, GROUP, CHIP), BF16),
            pltpu.VMEM((NA, 3, 2, CHIP, GROUP), BF16),
            pltpu.VMEM((NC, 3, GROUP, CHIP), BF16),
            pltpu.VMEM((NC, 3, 8, CHIP), F32),
            pltpu.VMEM((2, 3, GROUP, CHIP), BF16),
            pltpu.VMEM((2, 3, 8, CHIP), F32),
            pltpu.VMEM((CHIP, GROUP), BF16),
            pltpu.VMEM((dim // OUT // 2, CHIP, OUT), F32),
            pltpu.VMEM((NP, CHIP, OUT), F32),
            pltpu.VMEM((NP, ROWS, OUT), F32),
            pltpu.VMEM((2, ROWS, OUT), BF16),
            sem((SLOTS,)), sem((4,)), sem((4,)), sem((4,)),
            sem((NQ, 3)), sem((NQ, 3)),
            sem((2, 3)), sem((2, 3)), sem((NC, 3)), sem((NC, 3)),
            sem((NA, 3, 2)), sem((NA, 3, 2)),
            sem((NP,)), sem((NP,)), sem((2,)), sem,
        ],
        compiler_params=pltpu.CompilerParams(collective_id=0, has_side_effects=True, vmem_limit_bytes=67043328),
        name="layer",
    )(x, gain, cos, sin, wq, wk, wv, wo)


def solution(mesh):
    def step(x, gain, wq, wk, wv, wo):
        place = lax.div(lax.axis_index("sp"), 2) * CHIP + jnp.arange(CHIP)
        angle = place.astype(F32)[:, None] * THETA ** (-jnp.arange(HEAD // 2, dtype=F32) / (HEAD // 2))
        cos, sin = jnp.cos(angle), jnp.sin(angle)
        return _layer(x, gain[None], jnp.concatenate([cos, cos], 1), jnp.concatenate([-sin, sin], 1), wq, wk, wv, wo)

    tokens, whole = P(("dp", "sp"), None), P(None, None)
    return jax.shard_map(step, mesh=mesh, in_specs=(tokens, P(None), whole, whole, whole, whole), out_specs=tokens, check_vma=False)
```
